32 devices in a mesh: dp: 4 (over z), expert: 4 (over y, core), tensor: 2 (over x).
Axes of the slice: x: 2, y: 2, z: 4, core: 2. Of those that a mesh axis runs over, the one named last changes fastest.
Arguments:
- hidden: bfloat16 [2048, 6144], P(('dp', 'expert'), 'tensor'), may hold values from -6 to 6
- expert_ids: int32 [2048, 8], P(('dp', 'expert')), may hold values from 0 to 383, as said below
- gate_fixed: int32 [2048, 8], P(('dp', 'expert')), may hold values from 4096 to 65535
- slot_expert: int32 [16], replicated, may hold values from 0 to 383, as said below
- expert_in: bfloat16 [16, 6144, 2, 1024], P(('dp', 'expert'), 'tensor'), may hold values from -1 to 1, as said below
- expert_out: bfloat16 [16, 1024, 6144], P(('dp', 'expert'), None, 'tensor'), may hold values from -1 to 1, as said below
- shared_in: bfloat16 [6144, 2, 1024], P('tensor', None, 'dp'), may hold values from -0.078125 to 0.078125
- shared_out: bfloat16 [1024, 6144], P('dp', 'tensor'), may hold values from -0.1875 to 0.1875
Outputs:
- mixed: bfloat16 [2048, 6144], P(('dp', 'expert'), 'tensor')
The draws below stay inside these ranges and needn't reach their ends.
Inputs may be any that keep to these rules, and one draw needn't show every extreme that they name: `expert_ids`: each row names 8 different experts. `slot_expert`: 14 different experts fill the 16 slots; 2 of them hold two slots each, the others one. `expert_in`: slots that hold the same expert hold the same weights. `expert_out`: slots that hold the same expert hold the same weights.
All inputs are finite; a program needn't handle non-finite values.
Results may differ from the reference program's by a relative error of at most 0.006.
Values may be sent and summed in bfloat16 or wider, within the bound.
A program may use at most 192 MiB of HBM per device.

```python
import jax
import jax.numpy as jnp
from jax import lax

D = 6144
FF_E = 1024
FF_S = 1024
EXPERTS = 384
TOPK = 8
CAP = 4
TOK_DEV = 128
SLOTS = 16
REPL = 2
WIN = 14
TOKENS = 2048


def routing_plan(key):
    base = jax.random.fold_in(key, 4242)
    key_bias, key_noise, key_pick, key_perm = jax.random.split(base, 4)
    order = jnp.arange(EXPERTS, dtype=jnp.int32)
    level = jax.random.randint(key_bias, (EXPERTS,), 0, 8, dtype=jnp.int32)
    bias = level * level
    noise = jax.random.randint(key_noise, (TOKENS, EXPERTS), 0, 1024, dtype=jnp.int32)
    score = (noise + bias[None, :]) * EXPERTS + order[None, :]
    _, chosen = lax.top_k(score, TOPK)
    pick = jax.random.randint(key_pick, (EXPERTS,), 0, 1 << 20, dtype=jnp.int32) * EXPERTS + order
    ends = (order == 0) | (order == EXPERTS - 1)
    pick = jnp.where(ends, (1 << 21) * EXPERTS + order, pick).astype(jnp.int32)
    _, resident = lax.top_k(pick, WIN)
    heat = bias[resident] * EXPERTS + resident
    _, hot_place = lax.top_k(heat, REPL)
    entries = jnp.concatenate([jnp.arange(WIN, dtype=jnp.int32), hot_place.astype(jnp.int32)])
    shuffle = jax.random.permutation(key_perm, SLOTS)
    slot_resident = entries[shuffle]
    return (chosen.astype(jnp.int32), resident[slot_resident].astype(jnp.int32), slot_resident)


def expert_weights(key, salt, shape, fan_in):
    _, _, slot_resident = routing_plan(key)
    weight_key = jax.random.fold_in(key, salt)
    factor = fan_in ** (-0.5)

    def one_slot(resident_index):
        values = jax.random.truncated_normal(jax.random.fold_in(weight_key, resident_index), -4.0, 4.0, shape, jnp.float32)
        return (values * factor).astype(jnp.bfloat16)
    return lax.map(one_slot, slot_resident)


def draw_expert_ids(key, part):
    return routing_plan(key)[0]


def draw_slot_expert(key, part):
    return routing_plan(key)[1]


def draw_expert_in(key, part):
    return expert_weights(key, 17, (D, 2, FF_E), D)


def draw_expert_out(key, part):
    return expert_weights(key, 29, (FF_E, D), FF_E)


def touch_ends(array, own_key, low, high):
    dims = array.shape
    place = [jax.random.randint(jax.random.fold_in(own_key, axis), (), 0, dims[axis]) for axis in range(len(dims))]
    array = array.at[tuple(place)].set(low)
    longest = dims.index(max(dims))
    place[longest] = (place[longest] + 1) % dims[longest]
    return array.at[tuple(place)].set(high)


def steps_of(own_key, shape, cuts, smallest, high):
    def one(position, parts):
        heights = jax.random.uniform(jax.random.fold_in(jax.random.fold_in(own_key, 6), position), (parts,), jnp.float32, smallest / len(cuts), high / len(cuts))
        return jnp.repeat(jnp.exp(heights), shape[position] // parts).reshape((-1,) + (1,) * (len(shape) - position - 1))

    loudness = one(*cuts[0])
    for cut in cuts[1:]:
        loudness = loudness * one(*cut)
    return loudness


def scatter_about(rng, shape, width, bound, shards=(), kind=jnp.bfloat16):
    drawn = width * jax.random.normal(rng, shape, jnp.float32)
    if shards:
        drawn = drawn * steps_of(rng, shape, shards, -0.22, 0.18)
    return jnp.clip(drawn, -bound, bound).astype(kind)


def setup_inputs(seed: int = 0) -> dict:
    keys = jax.random.split(jax.random.key(seed), 9)
    hidden = scatter_about(keys[0], (TOKENS, D), 1.0, 6.0, ((0, 16), (1, 2)))
    expert_ids = draw_expert_ids(jax.random.fold_in(keys[8], 71), 0)
    gate_fixed = touch_ends(jax.random.randint(keys[2], (TOKENS, TOPK), 4096, 65536), jax.random.fold_in(keys[2], 1), 4096, 65535).astype(jnp.int32)
    slot_expert = draw_slot_expert(jax.random.fold_in(keys[8], 71), 0)
    expert_in = draw_expert_in(jax.random.fold_in(keys[8], 71), 0)
    expert_out = draw_expert_out(jax.random.fold_in(keys[8], 71), 0)
    shared_in = scatter_about(keys[6], (D, 2, FF_S), D ** -0.5, 0.078125, ((0, 2), (2, 4)))
    shared_out = scatter_about(keys[7], (FF_S, D), FF_S ** -0.5, 0.1875, ((0, 4), (1, 2)))
    return dict(hidden=hidden, expert_ids=expert_ids, gate_fixed=gate_fixed, slot_expert=slot_expert, expert_in=expert_in, expert_out=expert_out, shared_in=shared_in, shared_out=shared_out)


gate_scale = 1.0 / 65536.0


def swiglu(pre):
    return (jax.nn.silu(pre[:, 0, :]) * pre[:, 1, :]).astype(jnp.bfloat16)


def route_plan(chosen, row_rank, slot_expert):
    slot_count = slot_expert.shape[0]
    slot_iota = jnp.arange(slot_count, dtype=jnp.int32)[:, None]
    owns = slot_expert[:, None] == jnp.arange(chosen.shape[2], dtype=jnp.int32)[None, :]
    home = jnp.min(jnp.where(owns, slot_iota, slot_count), axis=0).astype(jnp.int32)
    spare = jnp.min(jnp.where(owns & (slot_iota != home[None, :]), slot_iota, slot_count), axis=0).astype(jnp.int32)
    home_of = jnp.sum(jnp.where(chosen, home[None, None, :], 0), axis=2).astype(jnp.int32)
    spare_of = jnp.sum(jnp.where(chosen, spare[None, None, :], 0), axis=2).astype(jnp.int32)
    first = row_rank < CAP
    spill = (row_rank >= CAP) & (row_rank < 2 * CAP) & (spare_of < slot_count)
    target = jnp.where(first, home_of, jnp.where(spill, spare_of, slot_count)).astype(jnp.int32)
    slot_row = jnp.where(first, row_rank, row_rank - CAP).astype(jnp.int32)
    return target, slot_row


def reference(hidden, expert_ids, gate_fixed, slot_expert, expert_in, expert_out, shared_in, shared_out):
    tokens_all = hidden.shape[0]
    slot_count = slot_expert.shape[0]
    blocks = tokens_all // TOK_DEV
    experts_iota = jnp.arange(EXPERTS, dtype=jnp.int32)
    chosen = expert_ids[:, :, None] == experts_iota[None, None, :]
    picked = jnp.any(chosen, axis=1).astype(jnp.int32).reshape(blocks, TOK_DEV, EXPERTS)
    before = (jnp.cumsum(picked, axis=1) - picked).astype(jnp.int32).reshape(tokens_all, EXPERTS)
    row_rank = jnp.sum(jnp.where(chosen, before[:, None, :], 0), axis=2).astype(jnp.int32)
    target, slot_row = route_plan(chosen, row_rank, slot_expert)
    token_iota = jnp.arange(tokens_all, dtype=jnp.int32)
    token_block = token_iota // TOK_DEV
    buffer_size = slot_count * blocks * CAP
    flat = jnp.where(target < slot_count, (target * blocks + token_block[:, None]) * CAP + slot_row, buffer_size).astype(jnp.int32)
    owner = jnp.broadcast_to(token_iota[:, None], flat.shape).astype(jnp.int32)
    table = jnp.full((buffer_size + 1,), tokens_all, jnp.int32).at[flat.reshape(-1)].set(owner.reshape(-1))
    table = table[:buffer_size].reshape(slot_count, blocks * CAP)
    padded = jnp.concatenate([hidden, jnp.zeros((1, D), hidden.dtype)], axis=0)

    def expert_pass(item):
        rows_index, weight_in, weight_out = item
        rows = padded[rows_index]
        pre = jnp.dot(rows, weight_in.reshape(D, 2 * FF_E), preferred_element_type=jnp.float32).reshape(-1, 2, FF_E)
        return jnp.dot(swiglu(pre), weight_out, preferred_element_type=jnp.float32).astype(jnp.bfloat16)

    answers = lax.map(expert_pass, (table, expert_in, expert_out)).reshape(buffer_size, D)
    answers = jnp.concatenate([answers, jnp.zeros((1, D), answers.dtype)], axis=0)
    gates = gate_fixed.astype(jnp.float32) * gate_scale
    routed = jnp.zeros((tokens_all, D), jnp.float32)
    for column in range(TOPK):
        routed = routed + gates[:, column:column + 1] * answers[flat[:, column]].astype(jnp.float32)
    shared_pre = jnp.dot(hidden, shared_in.reshape(D, 2 * FF_S), preferred_element_type=jnp.float32).reshape(-1, 2, FF_S)
    shared = jnp.dot(swiglu(shared_pre), shared_out, preferred_element_type=jnp.float32)
    return (shared + routed).astype(jnp.bfloat16)
```

```python
import functools

import jax
import jax.numpy as jnp
from jax import lax
from jax.experimental import pallas as pl
from jax.experimental.pallas import tpu as pltpu
from jax.sharding import PartitionSpec as P

CAP = 4
BLOCK = 2 * CAP
LANES = 128
TILE = 256
RING = 4
gate_scale = 1.0 / 65536.0
BF = jnp.bfloat16
F32 = jnp.float32
MESH = pl.DeviceIdType.MESH


def dot(a, b):
    return jnp.dot(a, b, preferred_element_type=F32)


def silu(v):
    return v / (1.0 + jnp.exp(-v))


def slot_plan(expert_ids, gate_fixed, slot_expert):
    tok_rows, topk_count = expert_ids.shape
    slot_count = slot_expert.shape[0]
    slot_iota = jnp.arange(slot_count, dtype=jnp.int32)
    same = slot_expert[:, None] == slot_expert[None, :]
    copy_of = jnp.sum((same & (slot_iota[None, :] < slot_iota[:, None])).astype(jnp.int32), axis=1)
    place = jnp.arange(BLOCK, dtype=jnp.int32) % CAP
    first_rank = (copy_of[:, None] * CAP + place[None, :]).reshape(-1)
    usable = jnp.repeat(copy_of < 2, BLOCK)
    column_expert = jnp.repeat(slot_expert, BLOCK)
    named = jnp.zeros((tok_rows, slot_count * BLOCK), jnp.bool_)
    gate = jnp.zeros((tok_rows, slot_count * BLOCK), jnp.int32)
    for k in range(topk_count):
        hit = expert_ids[:, k : k + 1] == column_expert[None, :]
        named = named | hit
        gate = jnp.where(hit, gate_fixed[:, k : k + 1], gate)
    token_iota = jnp.arange(tok_rows, dtype=jnp.int32)
    earlier = (token_iota[:, None] > token_iota[None, :]).astype(BF)
    before = jnp.dot(earlier, named.astype(BF), preferred_element_type=F32).astype(jnp.int32)
    served = named & usable[None, :] & (before == first_rank[None, :])
    gate = jnp.where(served, gate, 0)
    high = (gate // 256).astype(F32) * (256.0 * gate_scale)
    low = (gate % 256).astype(F32) * gate_scale
    return served.astype(BF), high.astype(BF), low.astype(BF)


def rows_of_words(weight):
    depth, _, units = weight.shape
    return weight.reshape(depth, 2, units // LANES, LANES).transpose(0, 2, 1, 3).reshape(-1, LANES)


def sorter(units):
    groups = units // LANES
    depth = TILE // (2 * groups)
    out = lax.broadcasted_iota(jnp.int32, (TILE, TILE), 0)
    inner = lax.broadcasted_iota(jnp.int32, (TILE, TILE), 1)
    shift = (2 * groups).bit_length() - 1
    d = lax.shift_right_logical(inner, jnp.int32(shift))
    j = lax.shift_right_logical(inner & (2 * groups - 1), jnp.int32(1))
    g = inner & 1
    return ((g * groups + j) * depth + d == out).astype(F32).astype(BF)


def kernel(
    sizes, served_ref, high_ref, low_ref, hid_ref, ae_ref, we_ref, as_ref, ws_ref, out_ref,
    hid2, send, arr, ans, ret, ring, wp_e, wo_e, raw_s, wp_s, wo_s,
    pm_own, pm_send, pm_recv, act_e, sp_own, sp_send, sp_recv, acts, act_send, acc,
    s_sem, r_sem, out_s, out_r, back_s, back_r, l_sem, ring_sem,
):
    E = sizes
    tok, D = hid_ref.shape
    D2 = D // 2
    R = served_ref.shape[1]
    N = R // BLOCK
    F = we_ref.shape[0]
    S = ws_ref.shape[0]
    z, e, t = lax.axis_index("dp"), lax.axis_index("expert"), lax.axis_index("tensor")
    me = z * E + e
    z1 = z + 1 - 2 * (z % 2)
    z2 = z + 2 - 4 * (z // 2)
    quarter = e % 4
    yy = (e // 2) % 2
    e_y = e + 2 - 4 * yy
    e_c = e + 1 - 2 * (e % 2)
    q_y = quarter + 2 - 4 * yy
    near = (z1, e, t)
    far = (z2, e, t)
    side = (z, e_y, t)
    twin = (z, e_c, t)
    other = (z, e, 1 - t)

    def load(index, src, dst):
        copy = pltpu.make_async_copy(src, dst, l_sem.at[index])
        copy.start()
        return copy

    load_hid = load(0, hid_ref, hid2.at[pl.ds(0, tok)])
    chunk = ring.shape[1]
    chunks = ae_ref.shape[0] // chunk

    def ring_copy(index):
        slot = index % RING
        return pltpu.make_async_copy(
            ae_ref.at[pl.ds(pl.multiple_of(index * chunk, chunk), chunk)], ring.at[slot], ring_sem.at[slot]
        )

    for index in range(min(RING, chunks)):
        ring_copy(index).start()
    load_raw = load(1, as_ref, raw_s.at[0])
    load_wo_e = load(2, we_ref, wo_e)
    load_wo_s = load(3, ws_ref, wo_s.at[0])

    def place_of(offset):
        slot = (me + offset) % N
        return slot, (slot // E, slot % E, t)

    barrier = pltpu.get_barrier_semaphore()

    @pl.loop(1, N)
    def _(offset):
        pl.semaphore_signal(barrier, inc=1, device_id=place_of(offset)[1], device_id_type=MESH)

    pl.semaphore_signal(barrier, inc=1, device_id=other, device_id_type=MESH)

    column = lax.broadcasted_iota(jnp.int32, (tok, R), 1)
    first_half = (column & CAP) == 0

    def halves(ref):
        value = ref[...].astype(F32)
        return jnp.where(first_half, value, 0.0).astype(BF), jnp.where(first_half, 0.0, value).astype(BF)

    load_hid.wait()
    pick = halves(served_ref)
    across = (((0,), (0,)), ((), ()))

    @pl.loop(0, D2 // TILE)
    def _(n):
        c = pl.multiple_of(n * TILE, TILE)
        c2 = pl.multiple_of(n * TILE + D2, TILE)
        rows = lax.dot_general(pick[0], hid2[pl.ds(0, tok), pl.ds(c, TILE)], across, preferred_element_type=F32)
        rows += lax.dot_general(pick[1], hid2[pl.ds(0, tok), pl.ds(c2, TILE)], across, preferred_element_type=F32)
        send[:, pl.ds(c, TILE)] = rows.astype(BF)

    pl.semaphore_wait(barrier, N)

    count = [0]

    def remote(src, dst, device):
        index = count[0]
        count[0] += 1
        return pltpu.make_async_remote_copy(
            src_ref=src, dst_ref=dst, send_sem=s_sem.at[index], recv_sem=r_sem.at[index],
            device_id=device, device_id_type=MESH,
        )

    def block_copy(src, dst, sends, recvs, offset):
        slot, device = place_of(offset)
        return pltpu.make_async_remote_copy(
            src_ref=src.at[pl.ds(pl.multiple_of(slot * BLOCK, BLOCK), BLOCK)],
            dst_ref=dst.at[pl.ds(pl.multiple_of(me * BLOCK, BLOCK), BLOCK)],
            send_sem=sends.at[offset], recv_sem=recvs.at[offset],
            device_id=device, device_id_type=MESH,
        )

    @pl.loop(1, N)
    def _(offset):
        block_copy(send, arr, out_s, out_r, offset).start()

    started = []

    def go(copy):
        copy.start()
        started.append(copy)
        return copy

    tokens = go(remote(hid_ref, hid2.at[pl.ds(tok, tok)], near))

    parts = 2
    q_rows = as_ref.shape[0] // 4
    p_rows = q_rows // parts
    o_rows = S // 4

    def in_rows(q, p):
        return pl.ds(pl.multiple_of(q * q_rows + p * p_rows, p_rows), p_rows)

    def out_rows(q):
        return pl.ds(pl.multiple_of(q * o_rows, o_rows), o_rows)

    w_in = [go(remote(as_ref.at[in_rows(quarter, p)], raw_s.at[1, in_rows(quarter, p)], far)) for p in range(parts)]
    w_out = [None] * 4
    w_out[1] = go(remote(ws_ref.at[out_rows(quarter)], wo_s.at[1, out_rows(quarter)], far))
    w_out[2] = go(remote(ws_ref.at[out_rows(quarter)], wo_s.at[2, out_rows(quarter)], near))

    def sort_rows(source, one_hot, units, row, store):
        groups = units // LANES
        depth = TILE // (2 * groups)
        pair = jnp.concatenate([source(row), source(row + TILE)], axis=1)
        mixed = dot(one_hot, pair).astype(BF)
        for g in range(2):
            for j in range(groups):
                at = (g * groups + j) * depth
                for half in range(2):
                    store(g, half * depth, depth, j, mixed[at : at + depth, half * LANES : (half + 1) * LANES])

    one_hot_e = sorter(F)
    depth_e = chunk // (2 * (F // LANES))

    @pl.loop(0, chunks)
    def _(index):
        slot = index % RING
        ring_copy(index).wait()

        @pl.loop(0, chunk // (2 * TILE))
        def _(pair):
            base = pl.multiple_of(index * depth_e + pair * (2 * TILE // (2 * (F // LANES))), 16)

            def store(g, first, depth, j, block):
                wp_e[g, pl.ds(pl.multiple_of(base + first, 16), depth), pl.ds(j * LANES, LANES)] = block

            def source(row):
                return ring[slot, pl.ds(pl.multiple_of(row, TILE), TILE), :]

            sort_rows(source, one_hot_e, F, pair * (2 * TILE), store)

        @pl.when(index + RING < chunks)
        def _():
            ring_copy(index + RING).start()

    def sort_shared(k):
        one_hot = sorter(S)
        step = 2 * TILE // (2 * (S // LANES))

        @pl.loop(0, as_ref.shape[0] // (2 * TILE))
        def _(pair):
            base = pl.multiple_of(pair * step, step)

            def store(g, first, depth, j, block):
                wp_s[k, g, pl.ds(pl.multiple_of(base + first, 16), depth), pl.ds(j * LANES, LANES)] = block

            def source(row):
                return raw_s[k, pl.ds(pl.multiple_of(row, TILE), TILE), :]

            sort_rows(source, one_hot, S, pair * (2 * TILE), store)

    load_raw.wait()
    sort_shared(0)

    row_of = lax.broadcasted_iota(jnp.int32, (R, TILE), 0)
    upper = (row_of & CAP) == 0
    mine = lax.shift_right_logical(row_of, jnp.int32(BLOCK.bit_length() - 1)) == me

    def own_block(whole, own):
        @pl.loop(0, D2 // TILE)
        def _(n):
            c = pl.ds(pl.multiple_of(n * TILE, TILE), TILE)
            whole[:, c] = jnp.where(mine, own[:, c].astype(F32), whole[:, c].astype(F32)).astype(BF)

    @pl.loop(1, N)
    def _(offset):
        block_copy(send, arr, out_s, out_r, offset).wait_recv()

    own_block(arr, send)

    mid = [remote(pm_send.at[n], pm_recv.at[n], other) for n in range(F // TILE)]
    for n in range(F // TILE):
        c = pl.ds(n * TILE, TILE)
        gate = dot(arr[...], wp_e[0, :D2, c]) + pltpu.roll(dot(arr[...], wp_e[0, D2:, c]), R - CAP, 0)
        up = pltpu.roll(dot(arr[...], wp_e[1, :D2, c]), CAP, 0) + dot(arr[...], wp_e[1, D2:, c])
        both = jnp.where(upper, gate, up)
        pm_own[n] = both
        pm_send[n] = both.astype(BF)
        go(mid[n])

    shared_mid = [remote(sp_send.at[k], sp_recv.at[k], other) for k in range(2)]
    act_back = [remote(act_send.at[k], acts.at[2 + k], near) for k in range(2)]

    def shared_up(k):
        for g in range(2):
            part = dot(hid2[...], wp_s[k, g])
            sp_own[k, g] = part
            sp_send[k, g] = part.astype(BF)
        go(shared_mid[k])

    def shared_act(k):
        shared_mid[k].wait_recv()
        gate = sp_own[k, 0] + sp_recv[k, 0].astype(F32)
        up = sp_own[k, 1] + sp_recv[k, 1].astype(F32)
        act = (silu(gate) * up).astype(BF)
        acts[k] = act[:tok]
        act_send[k] = act[tok:]
        go(act_back[k])

    tokens.wait_recv()
    shared_up(0)

    in_side = [remote(raw_s.at[1, in_rows(quarter, p)], raw_s.at[1, in_rows(quarter, p)], side) for p in range(parts)]
    in_twin = [remote(raw_s.at[1, in_rows(quarter, p)], raw_s.at[1, in_rows(quarter, p)], twin) for p in range(parts)]
    in_twin2 = [remote(raw_s.at[1, in_rows(q_y, p)], raw_s.at[1, in_rows(q_y, p)], twin) for p in range(parts)]
    out_side, out_twin, out_twin2 = {}, {}, {}
    for k in (1, 2, 3):
        rows, rows_y = wo_s.at[k, out_rows(quarter)], wo_s.at[k, out_rows(q_y)]
        out_side[k], out_twin[k], out_twin2[k] = remote(rows, rows, side), remote(rows, rows, twin), remote(rows_y, rows_y, twin)
    w_out[3] = remote(wo_s.at[1, out_rows(quarter)], wo_s.at[3, out_rows(quarter)], near)

    def spread_in(p):
        w_in[p].wait_recv()
        go(in_side[p])
        go(in_twin[p])

    def spread_out(k):
        w_out[k].wait_recv()
        go(out_side[k])
        go(out_twin[k])

    def pass_out(k):
        out_side[k].wait_recv()
        go(out_twin2[k])

    def have_out(k):
        out_twin[k].wait_recv()
        out_twin2[k].wait_recv()

    spread_in(0)

    load_wo_e.wait()
    for n in range(F // TILE):
        mid[n].wait_recv()
        total = pm_own[n] + pm_recv[n].astype(F32)
        act = silu(total) * pltpu.roll(total, R - CAP, 0)
        act_e[:, pl.ds(n * TILE, TILE)] = act.astype(BF)

    @pl.loop(0, D2 // TILE)
    def _(n):
        c = pl.multiple_of(n * TILE, TILE)
        c2 = pl.multiple_of(n * TILE + D2, TILE)
        one = dot(act_e[...], wo_e[:, pl.ds(c, TILE)])
        two = dot(act_e[...], wo_e[:, pl.ds(c2, TILE)])
        ans[:, pl.ds(c, TILE)] = jnp.where(upper, one, pltpu.roll(two, CAP, 0)).astype(BF)

    @pl.loop(1, N)
    def _(offset):
        block_copy(ans, ret, back_s, back_r, offset).start()

    spread_in(1)
    for p in range(2, parts):
        spread_in(p)
    shared_act(0)
    for p in range(parts):
        in_side[p].wait_recv()
        go(in_twin2[p])
    w_out[1].wait_recv()
    go(w_out[3])
    go(out_side[1])
    go(out_twin[1])
    spread_out(2)

    for p in range(parts):
        in_twin[p].wait_recv()
        in_twin2[p].wait_recv()
    sort_shared(1)
    shared_up(1)
    pass_out(1)
    pass_out(2)
    load_wo_s.wait()
    shared_act(1)
    have_out(1)

    @pl.loop(0, D // TILE)
    def _(n):
        c = pl.ds(pl.multiple_of(n * TILE, TILE), TILE)
        acc[:, c] = dot(acts[0], wo_s[0, :, c]) + dot(acts[1], wo_s[1, :, c])

    spread_out(3)

    @pl.loop(1, N)
    def _(offset):
        block_copy(ans, ret, back_s, back_r, offset).wait_recv()

    own_block(ret, ans)
    high, low = halves(high_ref), halves(low_ref)
    have_out(2)
    act_back[0].wait_recv()
    for half in range(2):
        @pl.loop(0, D2 // TILE)
        def _(n):
            c = pl.ds(pl.multiple_of(n * TILE + half * D2, TILE), TILE)
            back = ret[:, pl.ds(pl.multiple_of(n * TILE, TILE), TILE)]
            acc[:, c] += dot(acts[2], wo_s[2, :, c]) + dot(high[half], back) + dot(low[half], back)

    pass_out(3)
    act_back[1].wait_recv()
    have_out(3)

    @pl.loop(0, D // TILE)
    def _(n):
        c = pl.ds(pl.multiple_of(n * TILE, TILE), TILE)
        out_ref[:, c] = (acc[:, c] + dot(acts[3], wo_s[3, :, c])).astype(BF)

    @pl.loop(1, N)
    def _(offset):
        block_copy(send, arr, out_s, out_r, offset).wait_send()
        block_copy(ans, ret, back_s, back_r, offset).wait_send()

    for copy in started:
        copy.wait_send()


def solution(mesh):
    expert_size = mesh.shape["expert"]

    def shards(
        hidden, expert_ids, gate_fixed, slot_expert, expert_in, expert_out, shared_in, shared_out
    ):
        tok, D = hidden.shape
        F = expert_out.shape[1]
        S = shared_out.shape[0]
        N = slot_expert.shape[0]
        R = N * BLOCK
        served, high, low = slot_plan(expert_ids, gate_fixed, slot_expert)
        a_e = rows_of_words(expert_in[0])
        a_s = rows_of_words(shared_in)
        chunk = a_e.shape[0] // 16
        vmem = pl.BlockSpec(memory_space=pltpu.VMEM)
        hbm = pl.BlockSpec(memory_space=pl.ANY)
        dma = pltpu.SemaphoreType.DMA
        return pl.pallas_call(
            functools.partial(kernel, expert_size),
            out_shape=jax.ShapeDtypeStruct((tok, D), BF),
            in_specs=[vmem] * 3 + [hbm] * 5,
            out_specs=vmem,
            scratch_shapes=[
                pltpu.VMEM((2 * tok, D), BF),
                pltpu.VMEM((R, D // 2), BF),
                pltpu.VMEM((R, D // 2), BF),
                pltpu.VMEM((R, D // 2), BF),
                pltpu.VMEM((R, D // 2), BF),
                pltpu.VMEM((RING, chunk, LANES), BF),
                pltpu.VMEM((2, D, F), BF),
                pltpu.VMEM((F, D), BF),
                pltpu.VMEM((2, a_s.shape[0], LANES), BF),
                pltpu.VMEM((2, 2, D, S), BF),
                pltpu.VMEM((4, S, D), BF),
                pltpu.VMEM((F // TILE, R, TILE), F32),
                pltpu.VMEM((F // TILE, R, TILE), BF),
                pltpu.VMEM((F // TILE, R, TILE), BF),
                pltpu.VMEM((R, F), BF),
                pltpu.VMEM((2, 2, 2 * tok, S), F32),
                pltpu.VMEM((2, 2, 2 * tok, S), BF),
                pltpu.VMEM((2, 2, 2 * tok, S), BF),
                pltpu.VMEM((4, tok, S), BF),
                pltpu.VMEM((2, tok, S), BF),
                pltpu.VMEM((tok, D), F32),
                dma((64,)),
                dma((64,)),
                dma((N,)),
                dma((N,)),
                dma((N,)),
                dma((N,)),
                dma((4,)),
                dma((RING,)),
            ],
            compiler_params=pltpu.CompilerParams(
                collective_id=0, has_side_effects=True, vmem_limit_bytes=62 * 2**20
            ),
        )(served, high, low, hidden, a_e, expert_out[0], a_s, shared_out)

    in_specs = (
        P(("dp", "expert"), "tensor"),
        P(("dp", "expert"), None),
        P(("dp", "expert"), None),
        P(),
        P(("dp", "expert"), "tensor", None, None),
        P(("dp", "expert"), None, "tensor"),
        P("tensor", None, "dp"),
        P("dp", "tensor"),
    )
    out_specs = P(("dp", "expert"), "tensor")
    return jax.shard_map(
        shards, mesh=mesh, in_specs=in_specs, out_specs=out_specs, check_vma=False
    )
```

```python
import functools

import jax
import jax.numpy as jnp
from jax import lax
from jax.experimental import pallas as pl
from jax.experimental.pallas import tpu as pltpu
from jax.sharding import PartitionSpec as P

CAP = 4
BLOCK = 2 * CAP
LANES = 128
TILE = 256
RING = 4
gate_scale = 1.0 / 65536.0
BF = jnp.bfloat16
F32 = jnp.float32
MESH = pl.DeviceIdType.MESH


def dot(a, b):
    return jnp.dot(a, b, preferred_element_type=F32)


def silu(v):
    return v / (1.0 + jnp.exp(-v))


def rows_of_words(weight):
    depth, _, units = weight.shape
    return weight.reshape(depth, 2, units // LANES, LANES).transpose(0, 2, 1, 3).reshape(-1, LANES)


def sorter(units):
    groups = units // LANES
    depth = TILE // (2 * groups)
    out = lax.broadcasted_iota(jnp.int32, (TILE, TILE), 0)
    inner = lax.broadcasted_iota(jnp.int32, (TILE, TILE), 1)
    shift = (2 * groups).bit_length() - 1
    d = lax.shift_right_logical(inner, jnp.int32(shift))
    j = lax.shift_right_logical(inner & (2 * groups - 1), jnp.int32(1))
    g = inner & 1
    return ((g * groups + j) * depth + d == out).astype(F32).astype(BF)


def kernel(
    E, ids_hbm, fixed_hbm, slot_hbm, hid_ref, ae_ref, we_ref, as_ref, ws_ref, out_ref,
    ids_ref, fixed_ref, slot_ref, hid2, pick, high, low, send, arr, ans, ret, ring, wp_e, wo_e, raw_s, wp_s, wo_s,
    pm_own, pm_send, pm_recv, act_e, sp_own, sp_send, sp_recv, acts, act_send, acc,
    s_sem, r_sem, out_s, out_r, back_s, back_r, l_sem, ring_sem,
):
    tok, D = hid_ref.shape
    D2 = D // 2
    N = slot_ref.shape[1]
    R = N * BLOCK
    F = we_ref.shape[0]
    S = ws_ref.shape[0]
    z, e, t = lax.axis_index("dp"), lax.axis_index("expert"), lax.axis_index("tensor")
    me = z * E + e
    z1 = z + 1 - 2 * (z % 2)
    z2 = z + 2 - 4 * (z // 2)
    quarter = e % 4
    yy = (e // 2) % 2
    e_y = e + 2 - 4 * yy
    e_c = e + 1 - 2 * (e % 2)
    q_y = quarter + 2 - 4 * yy
    near = (z1, e, t)
    far = (z2, e, t)
    side = (z, e_y, t)
    twin = (z, e_c, t)
    other = (z, e, 1 - t)

    def load(index, src, dst):
        copy = pltpu.make_async_copy(src, dst, l_sem.at[index])
        copy.start()
        return copy

    load_small = [load(4, ids_hbm, ids_ref), load(5, fixed_hbm, fixed_ref), load(6, slot_hbm, slot_ref)]
    load_hid = load(0, hid_ref, hid2.at[pl.ds(0, tok)])
    chunk = ring.shape[1]
    chunks = ae_ref.shape[0] // chunk

    def ring_copy(index):
        slot = index % RING
        return pltpu.make_async_copy(
            ae_ref.at[pl.ds(pl.multiple_of(index * chunk, chunk), chunk)], ring.at[slot], ring_sem.at[slot]
        )

    def place_of(offset):
        slot = (me + offset) % N
        return slot, (slot // E, slot % E, t)

    barrier = pltpu.get_barrier_semaphore()

    @pl.loop(1, N)
    def _(offset):
        pl.semaphore_signal(barrier, inc=1, device_id=place_of(offset)[1], device_id_type=MESH)

    pl.semaphore_signal(barrier, inc=1, device_id=other, device_id_type=MESH)

    for index in range(min(RING, chunks)):
        ring_copy(index).start()
    load_raw = load(1, as_ref, raw_s.at[0])
    load_wo_e = load(2, we_ref, wo_e)
    load_wo_s = load(3, ws_ref, wo_s.at[0])

    for small in load_small:
        small.wait()
    with jax.named_scope("plan"):
        slot_of = lax.shift_right_logical(
            lax.broadcasted_iota(jnp.int32, (R, N), 0), jnp.int32(BLOCK.bit_length() - 1)
        )
        lane = lax.broadcasted_iota(jnp.int32, (R, N), 1)
        held = jnp.broadcast_to(slot_ref[...].astype(F32), (R, N))
        expert = jnp.sum(jnp.where(lane == slot_of, held, 0.0), axis=1, keepdims=True)
        copy_of = jnp.sum(jnp.where((held == expert) & (lane < slot_of), 1.0, 0.0), axis=1, keepdims=True)
        row = lax.broadcasted_iota(jnp.int32, (R, tok), 0)
        first_rank = copy_of * CAP + (row & (CAP - 1)).astype(F32)
        named = jnp.zeros((R, tok), F32)
        gate = jnp.zeros((R, tok), jnp.int32)
        for k in range(ids_ref.shape[0]):
            hit = jnp.broadcast_to(ids_ref[k : k + 1, :].astype(F32), (R, tok)) == expert
            named = jnp.where(hit, 1.0, named)
            gate = jnp.where(hit, jnp.broadcast_to(fixed_ref[k : k + 1, :], (R, tok)), gate)
        early = lax.broadcasted_iota(jnp.int32, (tok, tok), 0) < lax.broadcasted_iota(jnp.int32, (tok, tok), 1)
        before = dot(named.astype(BF), jnp.where(early, 1.0, 0.0).astype(BF))
        served = (named > 0.0) & (copy_of < 2.0) & (before == first_rank)
        gate = jnp.where(served, gate, 0)
        top = (row & CAP) == 0
        high_all = lax.shift_right_logical(gate, jnp.int32(8)).astype(F32) * (256.0 * gate_scale)
        low_all = (gate & 255).astype(F32) * gate_scale
        for half in range(2):
            keep = top if half == 0 else jnp.logical_not(top)
            pick[half] = jnp.where(served & keep, 1.0, 0.0).astype(BF)
            high[half] = jnp.where(keep, high_all, 0.0).astype(BF)
            low[half] = jnp.where(keep, low_all, 0.0).astype(BF)

    with jax.named_scope("gather_rows"):
        load_hid.wait()

        @pl.loop(0, D2 // TILE)
        def _(n):
            c = pl.multiple_of(n * TILE, TILE)
            c2 = pl.multiple_of(n * TILE + D2, TILE)
            rows = dot(pick[0], hid2[pl.ds(0, tok), pl.ds(c, TILE)])
            rows += dot(pick[1], hid2[pl.ds(0, tok), pl.ds(c2, TILE)])
            send[:, pl.ds(c, TILE)] = rows.astype(BF)

    with jax.named_scope("barrier"):
        pl.semaphore_wait(barrier, N)

    count = [0]

    def remote(src, dst, device):
        index = count[0]
        count[0] += 1
        return pltpu.make_async_remote_copy(
            src_ref=src, dst_ref=dst, send_sem=s_sem.at[index], recv_sem=r_sem.at[index],
            device_id=device, device_id_type=MESH,
        )

    def block_copy(src, dst, sends, recvs, offset):
        slot, device = place_of(offset)
        return pltpu.make_async_remote_copy(
            src_ref=src.at[pl.ds(pl.multiple_of(slot * BLOCK, BLOCK), BLOCK)],
            dst_ref=dst.at[pl.ds(pl.multiple_of(me * BLOCK, BLOCK), BLOCK)],
            send_sem=sends.at[offset], recv_sem=recvs.at[offset],
            device_id=device, device_id_type=MESH,
        )

    @pl.loop(1, N)
    def _(offset):
        block_copy(send, arr, out_s, out_r, offset).start()

    started = []

    def go(copy):
        copy.start()
        started.append(copy)
        return copy

    q_rows = as_ref.shape[0] // 4
    parts = max(p for p in (1, 2, 3) if q_rows % (2 * TILE * p) == 0)
    p_rows = q_rows // parts
    o_parts = 2
    o_rows = S // (4 * o_parts)
    pieces = [(k, p) for k in (1, 2, 3) for p in range(o_parts)]

    def in_rows(q, p):
        return pl.ds(pl.multiple_of(q * q_rows + p * p_rows, p_rows), p_rows)

    def out_rows(q, p):
        return pl.ds(pl.multiple_of((q * o_parts + p) * o_rows, o_rows), o_rows)

    def in_place(q, p, device):
        return remote(raw_s.at[1, in_rows(q, p)], raw_s.at[1, in_rows(q, p)], device)

    def out_place(k, q, p, device):
        return remote(wo_s.at[k, out_rows(q, p)], wo_s.at[k, out_rows(q, p)], device)

    w_out = {}

    def send_out(k, device):
        for p in range(o_parts):
            rows = out_rows(quarter, p)
            w_out[k, p] = go(remote(ws_ref.at[rows], wo_s.at[k, rows], device))

    send_out(1, far)
    send_out(2, near)
    tokens = go(remote(hid_ref, hid2.at[pl.ds(tok, tok)], near))
    w_in = [go(remote(as_ref.at[in_rows(quarter, p)], raw_s.at[1, in_rows(quarter, p)], far)) for p in range(parts)]
    for p in range(o_parts):
        rows = out_rows(quarter, p)
        w_out[3, p] = remote(wo_s.at[1, rows], wo_s.at[3, rows], near)
    in_side = [in_place(quarter, p, side) for p in range(parts)]
    in_twin = [in_place(quarter, p, twin) for p in range(parts)]
    in_twin2 = [in_place(q_y, p, twin) for p in range(parts)]
    out_side = {(k, p): out_place(k, quarter, p, side) for k, p in pieces}
    out_twin = {(k, p): out_place(k, quarter, p, twin) for k, p in pieces}
    out_twin2 = {(k, p): out_place(k, q_y, p, twin) for k, p in pieces}
    mid = [remote(pm_send.at[n], pm_recv.at[n], other) for n in range(F // TILE)]
    shared_mid = {(k, h): remote(sp_send.at[k, h], sp_recv.at[k, h], other) for k in range(2) for h in range(2)}
    act_back = [remote(act_send.at[k], acts.at[2 + k], near) for k in range(2)]

    def sort_rows(source, one_hot, units, row, store):
        groups = units // LANES
        depth = TILE // (2 * groups)
        pair = jnp.concatenate([source(row), source(row + TILE)], axis=1)
        mixed = dot(one_hot, pair).astype(BF)
        for g in range(2):
            for j in range(groups):
                at = (g * groups + j) * depth
                for half in range(2):
                    store(g, half * depth, depth, j, mixed[at : at + depth, half * LANES : (half + 1) * LANES])

    def sort_expert():
        one_hot = sorter(F)
        per_pair = 2 * TILE // (2 * (F // LANES))
        per_chunk = chunk // (2 * (F // LANES))
        pairs = chunk // (2 * TILE)
        together = 2 if pairs % 2 == 0 else 1

        @pl.loop(0, chunks)
        def _(index):
            slot = index % RING
            ring_copy(index).wait()

            @pl.loop(0, pairs // together)
            def _(step):
                for u in range(together):
                    pair = step * together + u
                    base = pl.multiple_of(index * per_chunk + pair * per_pair, 16)

                    def store(g, first, depth, j, block):
                        wp_e[g, pl.ds(pl.multiple_of(base + first, 16), depth), pl.ds(j * LANES, LANES)] = block

                    def source(row):
                        return ring[slot, pl.ds(pl.multiple_of(row, TILE), TILE), :]

                    sort_rows(source, one_hot, F, pair * (2 * TILE), store)

            @pl.when(index + RING < chunks)
            def _():
                ring_copy(index + RING).start()

    def sort_shared(k, first_pair, pairs):
        one_hot = sorter(S)
        per_pair = 2 * TILE // (2 * (S // LANES))
        together = 2 if pairs % 2 == 0 else 1

        @pl.loop(0, pairs // together)
        def _(step):
            for u in range(together):
                pair = first_pair + step * together + u
                base = pl.multiple_of(pair * per_pair, per_pair)

                def store(g, first, depth, j, block):
                    wp_s[k, g, pl.ds(pl.multiple_of(base + first, 16), depth), pl.ds(j * LANES, LANES)] = block

                def source(row):
                    return raw_s[k, pl.ds(pl.multiple_of(row, TILE), TILE), :]

                sort_rows(source, one_hot, S, pair * (2 * TILE), store)

    row_of = lax.broadcasted_iota(jnp.int32, (R, TILE), 0)
    upper = (row_of & CAP) == 0
    mine = lax.shift_right_logical(row_of, jnp.int32(BLOCK.bit_length() - 1)) == me

    def own_block(whole, own):
        @pl.loop(0, D2 // TILE)
        def _(n):
            c = pl.ds(pl.multiple_of(n * TILE, TILE), TILE)
            whole[:, c] = jnp.where(mine, own[:, c].astype(F32), whole[:, c].astype(F32)).astype(BF)

    def routed_up():
        @pl.loop(1, N)
        def _(offset):
            block_copy(send, arr, out_s, out_r, offset).wait_recv()

        own_block(arr, send)
        for n in range(F // TILE):
            c = pl.ds(n * TILE, TILE)
            gate = dot(arr[...], wp_e[0, :D2, c]) + pltpu.roll(dot(arr[...], wp_e[0, D2:, c]), R - CAP, 0)
            up = pltpu.roll(dot(arr[...], wp_e[1, :D2, c]), CAP, 0) + dot(arr[...], wp_e[1, D2:, c])
            both = jnp.where(upper, gate, up)
            pm_own[n] = both
            pm_send[n] = both.astype(BF)
            go(mid[n])

    def routed_down():
        load_wo_e.wait()
        for n in range(F // TILE):
            mid[n].wait_recv()
            total = pm_own[n] + pm_recv[n].astype(F32)
            act = silu(total) * pltpu.roll(total, R - CAP, 0)
            act_e[:, pl.ds(n * TILE, TILE)] = act.astype(BF)

        @pl.loop(0, D2 // TILE)
        def _(n):
            c = pl.multiple_of(n * TILE, TILE)
            c2 = pl.multiple_of(n * TILE + D2, TILE)
            one = dot(act_e[...], wo_e[:, pl.ds(c, TILE)])
            two = dot(act_e[...], wo_e[:, pl.ds(c2, TILE)])
            ans[:, pl.ds(c, TILE)] = jnp.where(upper, one, pltpu.roll(two, CAP, 0)).astype(BF)

        @pl.loop(1, N)
        def _(offset):
            block_copy(ans, ret, back_s, back_r, offset).start()

    def shared_up(k, h):
        for g in range(2):
            part = dot(hid2[h * tok : (h + 1) * tok, :], wp_s[k, g])
            sp_own[k, h, g] = part
            sp_send[k, h, g] = part.astype(BF)
        go(shared_mid[k, h])

    def shared_act(k, h):
        shared_mid[k, h].wait_recv()
        gate = sp_own[k, h, 0] + sp_recv[k, h, 0].astype(F32)
        up = sp_own[k, h, 1] + sp_recv[k, h, 1].astype(F32)
        act = (silu(gate) * up).astype(BF)
        if h == 0:
            acts[k] = act
        else:
            act_send[k] = act
            go(act_back[k])

    def spread_in(p):
        w_in[p].wait_recv()
        go(in_side[p])
        go(in_twin[p])

    def pass_in(p):
        in_side[p].wait_recv()
        go(in_twin2[p])

    def sort_in(p):
        in_twin[p].wait_recv()
        in_twin2[p].wait_recv()
        for q in range(4):
            sort_shared(1, (q * q_rows + p * p_rows) // (2 * TILE), p_rows // (2 * TILE))

    def spread_out(k, p):
        w_out[k, p].wait_recv()
        if k == 1:
            go(w_out[3, p])
        go(out_side[k, p])
        go(out_twin[k, p])

    def pass_out(k, p):
        out_side[k, p].wait_recv()
        go(out_twin2[k, p])

    def have_out(k):
        for p in range(o_parts):
            out_twin[k, p].wait_recv()
            out_twin2[k, p].wait_recv()

    wide = 2 * TILE

    def wide_tiles(width, body):
        @pl.loop(0, width // wide)
        def _(n):
            body(pl.multiple_of(n * wide, wide))

    def scope(name, function, *args):
        with jax.named_scope(name):
            function(*args)

    last = parts - 1
    scope("sort_e", sort_expert)
    scope("routed_up", routed_up)
    load_raw.wait()
    scope("sort_s0", sort_shared, 0, 0, as_ref.shape[0] // (2 * TILE))
    scope("shared_up00", shared_up, 0, 0)
    for p in range(o_parts):
        scope(f"spread_out1{p}", spread_out, 1, p)
    scope("routed_down", routed_down)
    for p in range(o_parts):
        scope(f"spread_out2{p}", spread_out, 2, p)
    scope("shared_act00", shared_act, 0, 0)
    for k in (1, 2):
        for p in range(o_parts):
            scope(f"pass_out{k}{p}", pass_out, k, p)
    for p in range(last):
        scope(f"spread_in{p}", spread_in, p)
        if p > 0:
            scope(f"pass_in{p - 1}", pass_in, p - 1)
    scope("wait_tokens", tokens.wait_recv)
    scope("shared_up01", shared_up, 0, 1)
    scope(f"spread_in{last}", spread_in, last)
    if last > 0:
        scope(f"pass_in{last - 1}", pass_in, last - 1)
    for p in range(last):
        scope(f"sort_in{p}", sort_in, p)
    scope("shared_act01", shared_act, 0, 1)
    scope(f"pass_in{last}", pass_in, last)
    scope("spread_out30", spread_out, 3, 0)
    scope(f"sort_in{last}", sort_in, last)
    scope("shared_up11", shared_up, 1, 1)
    scope("shared_up10", shared_up, 1, 0)
    for p in range(1, o_parts):
        scope(f"spread_out3{p}", spread_out, 3, p)
    scope("shared_act11", shared_act, 1, 1)
    scope("pass_out30", pass_out, 3, 0)
    scope("shared_act10", shared_act, 1, 0)
    load_wo_s.wait()
    scope("have_out1", have_out, 1)

    def first_sum(c):
        acc[:, pl.ds(c, wide)] = dot(acts[0], wo_s[0, :, pl.ds(c, wide)]) + dot(acts[1], wo_s[1, :, pl.ds(c, wide)])

    scope("first_sum", wide_tiles, D, first_sum)
    scope("have_out2", have_out, 2)
    scope("act_back0", act_back[0].wait_recv)

    def second_sum(c):
        acc[:, pl.ds(c, wide)] += dot(acts[2], wo_s[2, :, pl.ds(c, wide)])

    scope("second_sum", wide_tiles, D, second_sum)
    for p in range(1, o_parts):
        scope(f"pass_out3{p}", pass_out, 3, p)

    def returned():
        @pl.loop(1, N)
        def _(offset):
            block_copy(ans, ret, back_s, back_r, offset).wait_recv()

        own_block(ret, ans)

    scope("returned", returned)
    scope("act_back1", act_back[1].wait_recv)
    scope("have_out3", have_out, 3)
    across = (((0,), (0,)), ((), ()))

    def third_sum(half):
        def body(c):
            back = ret[:, pl.ds(c, wide)]
            at = pl.ds(pl.multiple_of(c + half * D2, wide), wide)
            routed = lax.dot_general(high[half], back, across, preferred_element_type=F32)
            routed += lax.dot_general(low[half], back, across, preferred_element_type=F32)
            out_ref[:, at] = (acc[:, at] + routed + dot(acts[3], wo_s[3, :, at])).astype(BF)

        wide_tiles(D2, body)

    for half in range(2):
        scope(f"third_sum{half}", third_sum, half)

    @pl.loop(1, N)
    def _(offset):
        block_copy(send, arr, out_s, out_r, offset).wait_send()
        block_copy(ans, ret, back_s, back_r, offset).wait_send()

    for copy in started:
        copy.wait_send()


def solution(mesh):
    expert_size = mesh.shape["expert"]

    def shards(
        hidden, expert_ids, gate_fixed, slot_expert, expert_in, expert_out, shared_in, shared_out
    ):
        tok, D = hidden.shape
        F = expert_out.shape[1]
        S = shared_out.shape[0]
        N, topk = slot_expert.shape[0], expert_ids.shape[1]
        R = N * BLOCK
        a_e = rows_of_words(expert_in[0])
        a_s = rows_of_words(shared_in)
        chunk = a_e.shape[0] // 16
        vmem = pl.BlockSpec(memory_space=pltpu.VMEM)
        hbm = pl.BlockSpec(memory_space=pltpu.HBM)
        dma = pltpu.SemaphoreType.DMA
        operands = (
            expert_ids.T, gate_fixed.T, slot_expert.reshape(1, N), hidden, a_e, expert_out[0], a_s, shared_out
        )
        return pl.pallas_call(
            functools.partial(kernel, expert_size),
            out_shape=jax.ShapeDtypeStruct((tok, D), BF),
            in_specs=[hbm] * 8,
            out_specs=vmem,
            scratch_shapes=[
                pltpu.VMEM((topk, tok), jnp.int32),
                pltpu.VMEM((topk, tok), jnp.int32),
                pltpu.VMEM((1, N), jnp.int32),
                pltpu.VMEM((2 * tok, D), BF),
                pltpu.VMEM((2, R, tok), BF),
                pltpu.VMEM((2, R, tok), BF),
                pltpu.VMEM((2, R, tok), BF),
                pltpu.VMEM((R, D // 2), BF),
                pltpu.VMEM((R, D // 2), BF),
                pltpu.VMEM((R, D // 2), BF),
                pltpu.VMEM((R, D // 2), BF),
                pltpu.VMEM((RING, chunk, LANES), BF),
                pltpu.VMEM((2, D, F), BF),
                pltpu.VMEM((F, D), BF),
                pltpu.VMEM((2, a_s.shape[0], LANES), BF),
                pltpu.VMEM((2, 2, D, S), BF),
                pltpu.VMEM((4, S, D), BF),
                pltpu.VMEM((F // TILE, R, TILE), F32),
                pltpu.VMEM((F // TILE, R, TILE), BF),
                pltpu.VMEM((F // TILE, R, TILE), BF),
                pltpu.VMEM((R, F), BF),
                pltpu.VMEM((2, 2, 2, tok, S), F32),
                pltpu.VMEM((2, 2, 2, tok, S), BF),
                pltpu.VMEM((2, 2, 2, tok, S), BF),
                pltpu.VMEM((4, tok, S), BF),
                pltpu.VMEM((2, tok, S), BF),
                pltpu.VMEM((tok, D), F32),
                dma((64,)),
                dma((64,)),
                dma((N,)),
                dma((N,)),
                dma((N,)),
                dma((N,)),
                dma((7,)),
                dma((RING,)),
            ],
            compiler_params=pltpu.CompilerParams(
                collective_id=0, has_side_effects=True, vmem_limit_bytes=46 * 2**20 + R * 28 * 2**10
            ),
        )(*(pltpu.with_memory_space_constraint(x, pltpu.HBM) for x in operands))

    in_specs = (
        P(("dp", "expert"), "tensor"),
        P(("dp", "expert"), None),
        P(("dp", "expert"), None),
        P(),
        P(("dp", "expert"), "tensor", None, None),
        P(("dp", "expert"), None, "tensor"),
        P("tensor", None, "dp"),
        P("dp", "tensor"),
    )
    out_specs = P(("dp", "expert"), "tensor")
    return jax.shard_map(
        shards, mesh=mesh, in_specs=in_specs, out_specs=out_specs, check_vma=False
    )
```
